32 devices in a mesh: dp: 4 (over z), seq: 4 (over y, core), tp: 2 (over x).
Axes of the slice: x: 2, y: 2, z: 4, core: 2. Of those that a mesh axis runs over, the one named last changes fastest.
Arguments:
- queries: bfloat16 [8192, 1024], P(('dp', 'seq'), 'tp'), parts along dimension 0, may hold values from -181 to 181
- rotated_key_states: bfloat16 [8192, 256], P(('dp', 'seq'), 'tp'), parts along dimension 0, may hold values from -6.1 to 6.1
- value_state_vectors: bfloat16 [8192, 256], P(('dp', 'seq'), 'tp'), parts along dimension 0, may hold values from -6 to 6
- out_weight: bfloat16 [1024, 8192], P('tp'), may hold values from -0.3125 to 0.3125
- residual: bfloat16 [8192, 8192], P(('dp', 'seq', 'tp')), parts along dimension 0, may hold values from -0.75 to 0.75
- norm_gain: bfloat16 [8192], replicated, may hold values from 0.099609375 to 2
Outputs:
- new_residual: bfloat16 [8192, 8192], P(('dp', 'seq', 'tp')), parts along dimension 0
- next_input: bfloat16 [8192, 8192], P(('dp', 'seq', 'tp')), parts along dimension 0
The draws below stay inside these ranges and needn't reach their ends.
There are 4 independent parts, one for each index of `dp`. The reference program is written for one: setup_inputs(seed, part) draws one part's arguments, and reference() takes and returns one part's arrays. A program takes and returns all parts, laid end to end along the dimension named above; an argument that names none is the same for every part. Nothing has to cross between parts.
All inputs are finite; a program needn't handle non-finite values.
Results may differ from the reference program's by a relative error of at most 0.025.
Values may be sent and summed in bfloat16 or wider, within the bound.
A program may use at most 192 MiB of HBM per device.

```python
import math
import jax
import jax.numpy as jnp
from jax import lax

D = 8192
HEAD_SIZE = 128
HQ_DEV = 4
QUERY_HEADS = 8
KEY_VALUE_HEADS = 2
SEQUENCE_TOKENS = 2048
N_TP = 2


def drawn_pair(key):
    query_key = jax.random.fold_in(key, 11)
    random_key_for_keys = jax.random.fold_in(key, 12)
    query_rows = 1.2 * jnp.clip(jax.random.normal(query_key, (SEQUENCE_TOKENS, QUERY_HEADS * HEAD_SIZE), jnp.float32), -5.0, 5.0)
    key_row_block = 1.2 * jnp.clip(jax.random.normal(random_key_for_keys, (SEQUENCE_TOKENS, KEY_VALUE_HEADS * HEAD_SIZE), jnp.float32), -5.0, 5.0)
    return (query_rows, key_row_block)


def draw_queries(key, part):
    return drawn_pair(key)[0].astype(jnp.bfloat16)


def draw_rotated_key_states(key, part):
    return drawn_pair(key)[1].astype(jnp.bfloat16)


def draw_out_weight(key, part):
    row_total = QUERY_HEADS * HEAD_SIZE
    entry_key = jax.random.fold_in(key, 31)
    factor_key = jax.random.fold_in(key, 32)
    entries = jnp.clip(jax.random.normal(entry_key, (row_total // 16, 16, D), jnp.float32), -5.0, 5.0)
    exponents = jax.random.uniform(factor_key, (row_total // 16, 1, D), jnp.float32, jnp.log(1.0 / 16.0), 0.0)
    factors = jnp.exp(exponents)
    group_count = QUERY_HEADS // HQ_DEV
    block_index = jnp.arange(row_total // 16, dtype=jnp.int32)
    group_index = block_index * 16 // (HQ_DEV * HEAD_SIZE)
    group_frac = group_index.astype(jnp.float32) / max(group_count - 1, 1)
    group_scale = jnp.exp(jnp.log(4.0) * (group_frac - 1.0)).reshape(row_total // 16, 1, 1)
    scaled = entries * factors * group_scale * (2.0 / row_total ** 0.5)
    return scaled.reshape(row_total, D).astype(jnp.bfloat16)


def block_levels(own_key, shape, cuts, low, top_value):
    loudness, own = 1.0, jax.random.fold_in(own_key, 6)
    for dim, shards_of in cuts:
        heights = jnp.exp(jax.random.uniform(jax.random.fold_in(own, dim), (shards_of,), jnp.float32, low / len(cuts), top_value / len(cuts)))
        loudness = loudness * jnp.repeat(heights, shape[dim] // shards_of).reshape([-1 if axis == dim else 1 for axis in range(len(shape))])
    return loudness


def gaussian(own_key, extent, scale, reach, cuts=(), kind=jnp.bfloat16):
    level = block_levels(own_key, extent, cuts, -0.22, 0.18) if cuts else 1.0
    array = jax.random.normal(own_key, extent, jnp.float32) * scale * level
    return jnp.minimum(jnp.maximum(array, -reach), reach).astype(kind)


def setup_inputs(seed: int = 0, part: int = 0) -> dict:
    arg_keys = jax.random.split(jax.random.key(seed), 7)
    own_keys = jax.random.split(jax.random.fold_in(arg_keys[6], part), 7)
    return {
        "queries": draw_queries(jax.random.fold_in(jax.random.fold_in(arg_keys[6], part), 71), part),
        "rotated_key_states": draw_rotated_key_states(jax.random.fold_in(jax.random.fold_in(arg_keys[6], part), 71), part),
        "value_state_vectors": gaussian(own_keys[2], (SEQUENCE_TOKENS, KEY_VALUE_HEADS * HEAD_SIZE), 1.0, 6.0, ((0, 4), (1, 2))),
        "out_weight": draw_out_weight(jax.random.fold_in(arg_keys[6], 71), part),
        "residual": gaussian(own_keys[4], (SEQUENCE_TOKENS, D), 0.05, 0.75, ((0, 8),)),
        "norm_gain": jnp.clip(jnp.exp(jax.random.uniform(arg_keys[5], (D,), jnp.float32, math.log(0.099609375), math.log(2.0))), 0.099609375, 2.0).astype(jnp.bfloat16),
    }


softness = 0.9
scale_floor = 256.0

def soft_grid(values):
    return values - softness * jnp.sin(jnp.pi * values) / jnp.pi

def fake_quant(blocks, block_axis, peak):
    block_max = lax.optimization_barrier(jnp.max(jnp.abs(blocks), axis=block_axis, keepdims=True))
    tensor_scale = peak / (6.0 * 448.0)
    block_scale = jnp.maximum(block_max / (6.0 * tensor_scale), scale_floor).astype(jnp.bfloat16)
    block_scale = lax.optimization_barrier(block_scale).astype(jnp.float32)
    spacing = block_scale * tensor_scale
    payload = soft_grid(blocks / spacing).astype(jnp.bfloat16)
    payload = lax.optimization_barrier(payload).astype(jnp.float32)
    return (payload * spacing).astype(jnp.bfloat16)

def reference(queries, rotated_key_states, value_state_vectors, out_weight, residual, norm_gain):
    score_scale = HEAD_SIZE ** (-0.5)
    grouped_heads = QUERY_HEADS // KEY_VALUE_HEADS
    q_heads = queries.reshape(SEQUENCE_TOKENS, QUERY_HEADS, HEAD_SIZE)
    key_heads = rotated_key_states.reshape(SEQUENCE_TOKENS, KEY_VALUE_HEADS, HEAD_SIZE)
    value_heads = value_state_vectors.reshape(SEQUENCE_TOKENS, KEY_VALUE_HEADS, HEAD_SIZE)
    positions = jnp.arange(SEQUENCE_TOKENS, dtype=jnp.int32)
    allowed = positions[:, None] >= positions[None, :]

    def one_head(head_index):
        q_one = lax.dynamic_index_in_dim(q_heads, head_index, 1, keepdims=False)
        kv_index = head_index // grouped_heads
        k_one = lax.dynamic_index_in_dim(key_heads, kv_index, 1, keepdims=False)
        v_one = lax.dynamic_index_in_dim(value_heads, kv_index, 1, keepdims=False)
        scores = jnp.dot(q_one, k_one.T, preferred_element_type=jnp.float32) * score_scale
        scores = jnp.where(allowed, scores, -jnp.inf)
        row_top = lax.optimization_barrier(jnp.max(scores, axis=1, keepdims=True))
        weights = jnp.exp(scores - row_top)
        totals = lax.optimization_barrier(jnp.sum(weights, axis=1, keepdims=True))
        attended = jnp.dot(weights.astype(jnp.bfloat16), v_one, preferred_element_type=jnp.float32) / totals
        return attended.astype(jnp.bfloat16)
    attended = lax.map(one_head, jnp.arange(QUERY_HEADS, dtype=jnp.int32))
    features = QUERY_HEADS * HEAD_SIZE
    act_t = attended.transpose(0, 2, 1).reshape(features, SEQUENCE_TOKENS).astype(jnp.float32)
    act_peak = jnp.max(jnp.abs(act_t))
    act_q = fake_quant(act_t.reshape(features // 16, 16, SEQUENCE_TOKENS), 1, act_peak).reshape(features, SEQUENCE_TOKENS)
    weight_f = out_weight.astype(jnp.float32)
    weight_peak = jnp.max(jnp.abs(weight_f))
    weight_q = fake_quant(weight_f.reshape(features // 16, 16, D), 1, weight_peak).reshape(features, D)
    group_width = features // N_TP
    projected = jnp.zeros((SEQUENCE_TOKENS, D), jnp.float32)
    for group_rank in range(N_TP):
        lower = group_rank * group_width
        partial_sum = lax.dot_general(act_q[lower:lower + group_width], weight_q[lower:lower + group_width], (((0,), (0,)), ((), ())), preferred_element_type=jnp.float32)
        partial_sum = lax.optimization_barrier(partial_sum.astype(jnp.bfloat16)).astype(jnp.float32)
        projected = projected + partial_sum
    hidden_sum = residual.astype(jnp.float32) + projected
    new_residual = hidden_sum.astype(jnp.bfloat16)
    mean_square = lax.optimization_barrier(jnp.mean(hidden_sum * hidden_sum, axis=1, keepdims=True))
    normed = hidden_sum * lax.rsqrt(mean_square + 1e-05) * norm_gain.astype(jnp.float32)
    norm_peak = jnp.max(jnp.abs(normed))
    next_input = fake_quant(normed.reshape(SEQUENCE_TOKENS, D // 16, 16), 2, norm_peak).reshape(SEQUENCE_TOKENS, D)
    return (new_residual, next_input)
```

```python
import functools

import jax
import jax.numpy as jnp
from jax import lax
from jax.experimental import pallas as pl
from jax.experimental.pallas import tpu as pltpu
from jax.sharding import PartitionSpec as P

HEAD_SIZE = 128
BLOCK = 16
softness = 0.9
scale_floor = 256.0
neg_large = -1e30
ROUND_BIG = 12582912.0
Q_COEFFS = (0.8999997814, -0.5804296733, 0.1500389216, -0.0212977078, 0.0016888914)


def soft_grid(u):
    turns = (u * 0.5 + ROUND_BIG) - ROUND_BIG
    t = u - (turns + turns)
    z = t * t
    q = jnp.float32(Q_COEFFS[-1])
    for c in Q_COEFFS[-2::-1]:
        q = q * z + jnp.float32(c)
    return u - (t - t * z) * q


def spacing_of(block_max, peak):
    tensor_scale = peak / (6.0 * 448.0)
    inv = 1.0 / (6.0 * tensor_scale)
    scale = jnp.maximum(block_max * inv, scale_floor).astype(jnp.bfloat16)
    return scale, tensor_scale


def quant_rows(x, peak):
    rows, cols = x.shape
    xb = x.reshape(rows // BLOCK, BLOCK, cols)
    block_max = jnp.max(jnp.abs(xb), axis=1, keepdims=True)
    scale, tensor_scale = spacing_of(block_max, peak)
    spacing = scale.astype(jnp.float32) * tensor_scale
    payload = soft_grid(xb * (1.0 / spacing)).astype(jnp.bfloat16).astype(jnp.float32)
    return (payload * spacing).reshape(rows, cols)


def quant_kernel(peak_ref, w_ref, out_ref, *, unroll):
    peak = peak_ref[0, 0]
    rows = w_ref.shape[0]

    def step(i, carry):
        sl = pl.ds(pl.multiple_of(i * BLOCK, BLOCK), BLOCK)
        out_ref[sl, :] = quant_rows(w_ref[sl, :].astype(jnp.float32), peak).astype(jnp.bfloat16)
        return carry

    lax.fori_loop(0, rows // BLOCK, step, 0, unroll=unroll)


def quant_weight(w, peak, width):
    rows, cols = w.shape
    return pl.pallas_call(
        functools.partial(quant_kernel, unroll=4),
        grid=(cols // width,),
        in_specs=[
            pl.BlockSpec(memory_space=pltpu.SMEM),
            pl.BlockSpec((rows, width), lambda i: (0, i)),
        ],
        out_specs=pl.BlockSpec((rows, width), lambda i: (0, i)),
        out_shape=jax.ShapeDtypeStruct((rows, cols), jnp.bfloat16),
        cost_estimate=pl.CostEstimate(
            flops=40 * rows * cols, bytes_accessed=4 * rows * cols, transcendentals=0
        ),
        name="quant_weight",
    )(peak, w)


def project_kernel(*refs, n_tp, n_feat):
    peak_ref, act_refs = refs[0], refs[1 : 1 + n_tp]
    own_ref, peer_ref, res_ref, gain_ref = refs[1 + n_tp : 5 + n_tp]
    new_ref, hid_ref, rstd_ref, top_ref = refs[5 + n_tp : 9 + n_tp]
    act_q, square_sum, row_top = refs[9 + n_tp :]
    step_id = pl.program_id(0)

    @pl.when(step_id == 0)
    def _():
        peak = peak_ref[0, 0]
        square_sum[...] = jnp.zeros_like(square_sum)
        row_top[...] = jnp.zeros_like(row_top)
        for k in range(n_tp):
            for lo in range(0, n_feat, 128):
                x = act_refs[k][lo : lo + 128, :].astype(jnp.float32)
                act_q[k, :, lo : lo + 128] = quant_rows(x, peak).T.astype(jnp.bfloat16)

    hidden = res_ref[...].astype(jnp.float32)
    for k in range(n_tp):
        w = own_ref[...] if k == 0 else peer_ref[0, k - 1]
        part = jnp.dot(act_q[k], w, preferred_element_type=jnp.float32)
        hidden = hidden + part.astype(jnp.bfloat16).astype(jnp.float32)
    new_ref[...] = hidden.astype(jnp.bfloat16)
    hid_ref[...] = hidden
    sq = square_sum[...]
    top = row_top[...]
    scaled = jnp.abs(hidden * gain_ref[...])
    for lo in range(0, hidden.shape[1], 128):
        part = hidden[:, lo : lo + 128]
        sq = sq + part * part
        top = jnp.maximum(top, scaled[:, lo : lo + 128])
    square_sum[...] = sq
    row_top[...] = top

    @pl.when(step_id == pl.num_programs(0) - 1)
    def _():
        width = hidden.shape[1] * pl.num_programs(0)
        mean_square = jnp.sum(square_sum[...], axis=1, keepdims=True) / width
        rstd = lax.rsqrt(mean_square + 1e-05)
        rstd_ref[...] = jnp.broadcast_to(rstd, rstd_ref.shape)
        top_all = jnp.max(jnp.max(row_top[...], axis=1, keepdims=True) * rstd)
        top_ref[...] = jnp.full(top_ref.shape, top_all, jnp.float32)


def project(peak, acts, w_own, w_peer, residual, gain):
    n_tp = len(acts)
    n_feat, tokens = acts[0].shape
    steps, _, _, width = w_peer.shape
    d = residual.shape[1]
    column = pl.BlockSpec((tokens, width), lambda i: (0, i))
    whole = pl.BlockSpec((tokens, 128), lambda i: (0, 0))
    return pl.pallas_call(
        functools.partial(project_kernel, n_tp=n_tp, n_feat=n_feat),
        grid=(steps,),
        in_specs=[pl.BlockSpec(memory_space=pltpu.SMEM)]
        + [pl.BlockSpec((n_feat, tokens), lambda i: (0, 0))] * n_tp
        + [
            pl.BlockSpec((n_feat, width), lambda i: (0, i)),
            pl.BlockSpec((1, n_tp - 1, n_feat, width), lambda i: (i, 0, 0, 0)),
            column,
            pl.BlockSpec((1, width), lambda i: (0, i)),
        ],
        out_specs=[column, column, whole, pl.BlockSpec((8, 128), lambda i: (0, 0))],
        out_shape=[
            jax.ShapeDtypeStruct((tokens, d), jnp.bfloat16),
            jax.ShapeDtypeStruct((tokens, d), jnp.float32),
            jax.ShapeDtypeStruct((tokens, 128), jnp.float32),
            jax.ShapeDtypeStruct((8, 128), jnp.float32),
        ],
        scratch_shapes=[
            pltpu.VMEM((n_tp, tokens, n_feat), jnp.bfloat16),
            pltpu.VMEM((tokens, 128), jnp.float32),
            pltpu.VMEM((tokens, 128), jnp.float32),
        ],
        cost_estimate=pl.CostEstimate(
            flops=2 * n_tp * n_feat * tokens * d, bytes_accessed=2 * n_tp * n_feat * d, transcendentals=0
        ),
        name="project",
    )(peak, *acts, w_own, w_peer, residual, gain)


def final_kernel(peak_ref, hid_ref, rstd_ref, gain_ref, out_ref):
    peak = peak_ref[0, 0]
    rows = hid_ref.shape[0]
    cols = hid_ref.shape[1]
    src = lax.broadcasted_iota(jnp.int32, (128, 128), 0)
    dst = lax.broadcasted_iota(jnp.int32, (128, 128), 1)
    spread = jnp.where(src == (dst // BLOCK) * BLOCK + BLOCK - 1, 1.0, 0.0).astype(jnp.bfloat16)
    rstd = rstd_ref[...]
    for lo in range(0, cols, 128):
        x = hid_ref[:, lo : lo + 128] * rstd * gain_ref[:, lo : lo + 128]
        m = jnp.abs(x)
        for s in (1, 2, 4, 8):
            m = jnp.maximum(m, pltpu.roll(m, s, 1))
        scale, tensor_scale = spacing_of(m, peak)
        scale = jnp.dot(scale, spread, preferred_element_type=jnp.float32)
        spacing = scale * tensor_scale
        payload = soft_grid(x / spacing).astype(jnp.bfloat16).astype(jnp.float32)
        out_ref[:, lo : lo + 128] = (payload * spacing).astype(jnp.bfloat16)


def final_quant(peak, hidden, rstd, gain):
    tokens, d = hidden.shape
    width = 1024
    rows = min(64, tokens)
    column = pl.BlockSpec((rows, width), lambda i, j: (i, j))
    return pl.pallas_call(
        final_kernel,
        grid=(tokens // rows, d // width),
        in_specs=[
            pl.BlockSpec(memory_space=pltpu.SMEM),
            column,
            pl.BlockSpec((rows, 128), lambda i, j: (i, 0)),
            pl.BlockSpec((1, width), lambda i, j: (0, j)),
        ],
        out_specs=column,
        out_shape=jax.ShapeDtypeStruct((tokens, d), jnp.bfloat16),
        name="final_quant",
    )(peak, hidden, rstd, gain)


def attend(queries, keys, values, first_query):
    token_count = queries.shape[0]
    kv_heads = keys.shape[1] // HEAD_SIZE
    grouped = queries.shape[1] // HEAD_SIZE // kv_heads
    q = queries.reshape(token_count, kv_heads, grouped, HEAD_SIZE)
    k = keys.reshape(-1, kv_heads, HEAD_SIZE)
    v = values.reshape(-1, kv_heads, HEAD_SIZE)
    scores = jnp.einsum("tkgd,skd->kgts", q, k, preferred_element_type=jnp.float32)
    scores = scores * HEAD_SIZE ** (-0.5)
    query_pos = first_query + lax.broadcasted_iota(jnp.int32, (token_count, 1), 0)
    key_pos = lax.broadcasted_iota(jnp.int32, (1, k.shape[0]), 1)
    allowed = query_pos >= key_pos
    masked = jnp.where(allowed, scores, neg_large)
    top = jnp.max(masked, axis=3, keepdims=True)
    weights = jnp.where(allowed, jnp.exp(masked - top), 0.0)
    total = jnp.sum(weights, axis=3)
    summed = jnp.einsum(
        "kgts,skd->kgtd", weights.astype(jnp.bfloat16), v, preferred_element_type=jnp.float32
    )
    attended = (summed / total[..., None]).astype(jnp.bfloat16)
    return attended.transpose(0, 1, 3, 2).reshape(-1, token_count)


def local(queries, keys, values, out_weight, residual, norm_gain):
    token_count = queries.shape[0]
    n_tp = lax.axis_size("tp")
    tp_rank = lax.axis_index("tp")
    slabs = lax.axis_size("dp") * lax.axis_size("seq")
    d = out_weight.shape[1]
    width = d // slabs
    kv = lax.all_gather(jnp.stack((keys, values)), "seq", axis=1, tiled=True)

    weight_top = jnp.max(jnp.abs(out_weight)).astype(jnp.float32)
    weight_peak = lax.pmax(weight_top, "tp").reshape(1, 1)
    slab_id = lax.axis_index("dp") * lax.axis_size("seq") + lax.axis_index("seq")
    slab = lax.dynamic_slice_in_dim(out_weight, slab_id * width, width, axis=1)
    slab_q = quant_weight(slab, weight_peak, width)
    shifts = [[(i, (i + k) % n_tp) for i in range(n_tp)] for k in range(1, n_tp)]
    from_peers = jnp.stack([lax.ppermute(slab_q, "tp", ring) for ring in shifts])
    w_peer = lax.all_gather(from_peers, ("dp", "seq"), axis=0)
    w_own = quant_weight(out_weight, weight_peak, width)

    act_t = attend(queries, kv[0], kv[1], lax.axis_index("seq") * token_count)
    act_top = jnp.max(jnp.abs(act_t)).astype(jnp.float32)
    share = token_count // n_tp
    pieces = []
    for k in range(n_tp):
        whose = lax.rem(tp_rank + k, n_tp)
        piece = lax.dynamic_slice_in_dim(act_t, whose * share, share, axis=1)
        pieces.append(piece if k == 0 else lax.ppermute(piece, "tp", shifts[k - 1]))
    act_peak = lax.pmax(act_top, ("seq", "tp")).reshape(1, 1)

    gain = norm_gain.astype(jnp.float32).reshape(1, d)
    new_residual, hidden, rstd, top = project(act_peak, pieces, w_own, w_peer, residual, gain)
    norm_peak = lax.pmax(top[0, 0], ("seq", "tp")).reshape(1, 1)
    next_input = final_quant(norm_peak, hidden, rstd, gain)
    return (new_residual, next_input)


def solution(mesh):
    in_specs = (
        P(("dp", "seq"), "tp"),
        P(("dp", "seq"), "tp"),
        P(("dp", "seq"), "tp"),
        P("tp", None),
        P(("dp", "seq", "tp"), None),
        P(),
    )
    out_specs = (P(("dp", "seq", "tp"), None), P(("dp", "seq", "tp"), None))
    return jax.shard_map(local, mesh=mesh, in_specs=in_specs, out_specs=out_specs, check_vma=False)
```

```python
import functools

import jax
import jax.numpy as jnp
from jax import lax
from jax.experimental import pallas as pl
from jax.experimental.pallas import tpu as pltpu
from jax.sharding import PartitionSpec as P

HEAD_SIZE = 128
BLOCK = 16
softness = 0.9
scale_floor = 256.0
neg_large = -1e30
ROUND_BIG = 12582912.0
Q_COEFFS = (0.8999997814, -0.5804296733, 0.1500389216, -0.0212977078, 0.0016888914)


def soft_grid(u):
    turns = (u * 0.5 + ROUND_BIG) - ROUND_BIG
    t = u - (turns + turns)
    z = t * t
    q = jnp.float32(Q_COEFFS[-1])
    for c in Q_COEFFS[-2::-1]:
        q = q * z + jnp.float32(c)
    return u - (t - t * z) * q


def spacing_of(block_max, peak):
    tensor_scale = peak / (6.0 * 448.0)
    inv = 1.0 / (6.0 * tensor_scale)
    scale = jnp.maximum(block_max * inv, scale_floor).astype(jnp.bfloat16)
    return scale, tensor_scale


def quant_rows(x, peak):
    rows, cols = x.shape
    xb = x.reshape(rows // BLOCK, BLOCK, cols)
    block_max = jnp.max(jnp.abs(xb), axis=1, keepdims=True)
    scale, tensor_scale = spacing_of(block_max, peak)
    spacing = scale.astype(jnp.float32) * tensor_scale
    payload = soft_grid(xb * (1.0 / spacing)).astype(jnp.bfloat16).astype(jnp.float32)
    return (payload * spacing).reshape(rows, cols)


def quant_kernel(peak_ref, w_ref, out_ref, *, unroll):
    peak = peak_ref[0, 0]
    rows = w_ref.shape[0]

    def step(i, carry):
        sl = pl.ds(pl.multiple_of(i * BLOCK, BLOCK), BLOCK)
        out_ref[sl, :] = quant_rows(w_ref[sl, :].astype(jnp.float32), peak).astype(jnp.bfloat16)
        return carry

    lax.fori_loop(0, rows // BLOCK, step, 0, unroll=unroll)


def quant_weight(w, peak, width, first, cols):
    rows = w.shape[0]
    skip = first // width
    return pl.pallas_call(
        functools.partial(quant_kernel, unroll=4),
        grid=(cols // width,),
        in_specs=[
            pl.BlockSpec(memory_space=pltpu.SMEM),
            pl.BlockSpec((rows, width), lambda i: (0, i + skip)),
        ],
        out_specs=pl.BlockSpec((rows, width), lambda i: (0, i)),
        out_shape=jax.ShapeDtypeStruct((rows, cols), jnp.bfloat16),
        cost_estimate=pl.CostEstimate(
            flops=40 * rows * cols, bytes_accessed=4 * rows * cols, transcendentals=0
        ),
        name="quant_weight",
    )(peak, w)


def project_kernel(*refs, n_tp, n_feat, n_alias, features):
    peak_ref, act_refs = refs[0], refs[1 : 1 + n_tp]
    own_ref, peer_ref, res_ref, gain_ref, sq_in, top_in = refs[1 + n_tp : 7 + n_tp]
    refs = refs[7 + n_tp + n_alias :]
    new_ref, hid_ref, square_sum, row_top, rstd_ref, top_ref, act_q = refs
    step_id = pl.program_id(0)

    @pl.when(step_id == 0)
    def _():
        peak = peak_ref[0, 0]
        square_sum[...] = sq_in[...]
        row_top[...] = top_in[...]
        for k in range(n_tp):
            for lo in range(0, n_feat, 128):
                x = act_refs[k][lo : lo + 128, :].astype(jnp.float32)
                act_q[k, :, lo : lo + 128] = quant_rows(x, peak).T.astype(jnp.bfloat16)

    hidden = res_ref[...].astype(jnp.float32)
    for k in range(n_tp):
        w = own_ref[...] if k == 0 else peer_ref[0, k - 1]
        part = jnp.dot(act_q[k], w, preferred_element_type=jnp.float32)
        hidden = hidden + part.astype(jnp.bfloat16).astype(jnp.float32)
    new_ref[...] = hidden.astype(jnp.bfloat16)
    hid_ref[...] = hidden
    sq = square_sum[...]
    top = row_top[...]
    scaled = jnp.abs(hidden * gain_ref[...])
    for lo in range(0, hidden.shape[1], 128):
        part = hidden[:, lo : lo + 128]
        sq = sq + part * part
        top = jnp.maximum(top, scaled[:, lo : lo + 128])
    square_sum[...] = sq
    row_top[...] = top

    @pl.when(step_id == pl.num_programs(0) - 1)
    def _():
        mean_square = jnp.sum(square_sum[...], axis=1, keepdims=True) / features
        rstd = lax.rsqrt(mean_square + 1e-05)
        rstd_ref[...] = jnp.broadcast_to(rstd, rstd_ref.shape)
        top_all = jnp.max(jnp.max(row_top[...], axis=1, keepdims=True) * rstd)
        top_ref[...] = jnp.full(top_ref.shape, top_all, jnp.float32)


def project(peak, acts, w_own, w_peer, residual, gain, stats, width, skip, wide, made):
    n_tp = len(acts)
    n_feat, tokens = acts[0].shape
    d = residual.shape[1]
    steps = w_own.shape[1] // width
    column = pl.BlockSpec((tokens, width), lambda i: (0, i + skip))
    whole = pl.BlockSpec((tokens, 128), lambda i: (0, 0))
    if wide:
        peer_spec = pl.BlockSpec((1, n_tp - 1, n_feat, width), lambda i: (0, 0, 0, i))
    else:
        peer_spec = pl.BlockSpec((1, n_tp - 1, n_feat, width), lambda i: (i, 0, 0, 0))
    stat = jax.ShapeDtypeStruct((tokens, 128), jnp.float32)
    return pl.pallas_call(
        functools.partial(project_kernel, n_tp=n_tp, n_feat=n_feat, n_alias=len(made), features=d),
        grid=(steps,),
        in_specs=[pl.BlockSpec(memory_space=pltpu.SMEM)]
        + [pl.BlockSpec((n_feat, tokens), lambda i: (0, 0))] * n_tp
        + [
            pl.BlockSpec((n_feat, width), lambda i: (0, i)),
            peer_spec,
            column,
            pl.BlockSpec((1, width), lambda i: (0, i + skip)),
            whole,
            whole,
        ]
        + [pl.BlockSpec(memory_space=pl.ANY)] * len(made),
        out_specs=[column, column, whole, whole, whole, pl.BlockSpec((8, 128), lambda i: (0, 0))],
        out_shape=[
            jax.ShapeDtypeStruct((tokens, d), jnp.bfloat16),
            jax.ShapeDtypeStruct((tokens, d), jnp.float32),
            stat,
            stat,
            stat,
            jax.ShapeDtypeStruct((8, 128), jnp.float32),
        ],
        input_output_aliases={7 + n_tp + i: i for i in range(len(made))},
        scratch_shapes=[pltpu.VMEM((n_tp, tokens, n_feat), jnp.bfloat16)],
        cost_estimate=pl.CostEstimate(
            flops=2 * n_tp * n_feat * tokens * steps * width,
            bytes_accessed=2 * n_tp * n_feat * steps * width,
            transcendentals=0,
        ),
        name="project",
    )(peak, *acts, w_own, w_peer, residual, gain, *stats, *made)


def final_kernel(peak_ref, hid_ref, rstd_ref, gain_ref, out_ref, narrow, wide):
    peak = peak_ref[0, 0]
    rows, cols = hid_ref.shape
    src = lax.broadcasted_iota(jnp.int32, (128, 128), 0)
    dst = lax.broadcasted_iota(jnp.int32, (128, 128), 1)
    spread = jnp.where(src == (dst // BLOCK) * BLOCK + BLOCK - 1, 1.0, 0.0).astype(jnp.bfloat16)
    rstd = rstd_ref[...]
    tensor_scale = peak / (6.0 * 448.0)
    pieces = cols // 128
    for i in range(pieces):
        x = hid_ref[:, i * 128 : i * 128 + 128] * rstd * gain_ref[:, i * 128 : i * 128 + 128]
        m = jnp.abs(x)
        for s in (1, 2, 4, 8):
            m = jnp.maximum(m, pltpu.roll(m, s, 1))
        narrow[i * rows : (i + 1) * rows, :] = spacing_of(m, peak)[0]
    wide[...] = jnp.dot(narrow[...], spread, preferred_element_type=jnp.float32)
    for i in range(pieces):
        x = hid_ref[:, i * 128 : i * 128 + 128] * rstd * gain_ref[:, i * 128 : i * 128 + 128]
        spacing = wide[i * rows : (i + 1) * rows, :] * tensor_scale
        payload = soft_grid(x * pl.reciprocal(spacing)).astype(jnp.bfloat16).astype(jnp.float32)
        out_ref[:, i * 128 : i * 128 + 128] = (payload * spacing).astype(jnp.bfloat16)


def final_quant(peak, hidden, rstd, gain):
    tokens, d = hidden.shape
    width = 2048
    rows = min(64, tokens)
    column = pl.BlockSpec((rows, width), lambda i, j: (i, j))
    return pl.pallas_call(
        final_kernel,
        grid=(tokens // rows, d // width),
        in_specs=[
            pl.BlockSpec(memory_space=pltpu.SMEM),
            column,
            pl.BlockSpec((rows, 128), lambda i, j: (i, 0)),
            pl.BlockSpec((1, width), lambda i, j: (0, j)),
        ],
        out_specs=column,
        out_shape=jax.ShapeDtypeStruct((tokens, d), jnp.bfloat16),
        scratch_shapes=[
            pltpu.VMEM((rows * width // 128, 128), jnp.bfloat16),
            pltpu.VMEM((rows * width // 128, 128), jnp.float32),
        ],
        name="final_quant",
    )(peak, hidden, rstd, gain)


def attend(queries, keys, values, first_query):
    token_count = queries.shape[0]
    kv_heads = keys.shape[1] // HEAD_SIZE
    grouped = queries.shape[1] // HEAD_SIZE // kv_heads
    q = queries.reshape(token_count, kv_heads, grouped, HEAD_SIZE)
    k = keys.reshape(-1, kv_heads, HEAD_SIZE)
    v = values.reshape(-1, kv_heads, HEAD_SIZE)
    scores = jnp.einsum("tkgd,skd->kgts", q, k, preferred_element_type=jnp.float32)
    scores = scores * HEAD_SIZE ** (-0.5)
    query_pos = first_query + lax.broadcasted_iota(jnp.int32, (token_count, 1), 0)
    key_pos = lax.broadcasted_iota(jnp.int32, (1, k.shape[0]), 1)
    allowed = query_pos >= key_pos
    masked = jnp.where(allowed, scores, neg_large)
    top = jnp.max(masked, axis=3, keepdims=True)
    weights = jnp.where(allowed, jnp.exp(masked - top), 0.0)
    total = jnp.sum(weights, axis=3)
    summed = jnp.einsum(
        "kgts,skd->kgtd", weights.astype(jnp.bfloat16), v, preferred_element_type=jnp.float32
    )
    attended = (summed / total[..., None]).astype(jnp.bfloat16)
    return attended.transpose(0, 1, 3, 2).reshape(-1, token_count)


def local(queries, keys, values, out_weight, residual, norm_gain):
    token_count = queries.shape[0]
    n_tp = lax.axis_size("tp")
    tp_rank = lax.axis_index("tp")
    slabs = lax.axis_size("dp") * lax.axis_size("seq")
    d = out_weight.shape[1]
    width = d // slabs
    kv = lax.all_gather(jnp.stack((keys, values)), "seq", axis=1, tiled=True)

    weight_top = jnp.max(jnp.abs(out_weight)).astype(jnp.float32)
    weight_peak = lax.pmax(weight_top, "tp").reshape(1, 1)
    slab_id = lax.axis_index("dp") * lax.axis_size("seq") + lax.axis_index("seq")
    direct = 128
    gather_w = width - direct
    gathered = slabs * gather_w
    slab = lax.dynamic_slice_in_dim(out_weight, slab_id * gather_w, gather_w, axis=1)
    slab_q = quant_weight(slab, weight_peak, gather_w, 0, gather_w)
    shifts = [[(i, (i + k) % n_tp) for i in range(n_tp)] for k in range(1, n_tp)]
    from_peers = jnp.stack([lax.ppermute(slab_q, "tp", ring) for ring in shifts])
    w_peer = lax.all_gather(from_peers, ("dp", "seq"), axis=0)
    near_own = quant_weight(out_weight, weight_peak, 512, gathered, d - gathered)
    near_peer = jnp.stack([lax.ppermute(near_own, "tp", ring) for ring in shifts])[None]
    w_own = quant_weight(out_weight, weight_peak, gather_w, 0, gathered)

    act_t = attend(queries, kv[0], kv[1], lax.axis_index("seq") * token_count)
    act_top = jnp.max(jnp.abs(act_t)).astype(jnp.float32)
    share = token_count // n_tp
    pieces = []
    for k in range(n_tp):
        whose = lax.rem(tp_rank + k, n_tp)
        piece = lax.dynamic_slice_in_dim(act_t, whose * share, share, axis=1)
        pieces.append(piece if k == 0 else lax.ppermute(piece, "tp", shifts[k - 1]))
    act_peak = lax.pmax(act_top, ("seq", "tp")).reshape(1, 1)

    gain = norm_gain.astype(jnp.float32).reshape(1, d)
    stats = (jnp.zeros((share, 128), jnp.float32),) * 2
    near = project(
        act_peak, pieces, near_own, near_peer, residual, gain, stats, 512, gathered // 512, True, ()
    )
    new_residual, hidden, _, _, rstd, top = project(
        act_peak, pieces, w_own, w_peer, residual, gain, near[2:4], gather_w, 0, False, near[:2]
    )
    norm_peak = lax.pmax(top[0, 0], ("seq", "tp")).reshape(1, 1)
    next_input = final_quant(norm_peak, hidden, rstd, gain)
    return (new_residual, next_input)


def solution(mesh):
    in_specs = (
        P(("dp", "seq"), "tp"),
        P(("dp", "seq"), "tp"),
        P(("dp", "seq"), "tp"),
        P("tp", None),
        P(("dp", "seq", "tp"), None),
        P(),
    )
    out_specs = (P(("dp", "seq", "tp"), None), P(("dp", "seq", "tp"), None))
    return jax.shard_map(local, mesh=mesh, in_specs=in_specs, out_specs=out_specs, check_vma=False)
```

```python
import functools

import jax
import jax.numpy as jnp
from jax import lax
from jax.experimental import pallas as pl
from jax.experimental.pallas import tpu as pltpu
from jax.sharding import PartitionSpec as P

HEAD_SIZE = 128
BLOCK = 16
softness = 0.9
scale_floor = 256.0
neg_large = -1e30
ROUND_BIG = 12582912.0
Q_COEFFS = (0.8999997814, -0.5804296733, 0.1500389216, -0.0212977078, 0.0016888914)


def soft_grid(u):
    turns = (u * 0.5 + ROUND_BIG) - ROUND_BIG
    t = u - (turns + turns)
    z = t * t
    q = jnp.float32(Q_COEFFS[-1])
    for c in Q_COEFFS[-2::-1]:
        q = q * z + jnp.float32(c)
    return u - (t - t * z) * q


def spacing_of(block_max, peak):
    tensor_scale = peak / (6.0 * 448.0)
    inv = 1.0 / (6.0 * tensor_scale)
    scale = jnp.maximum(block_max * inv, scale_floor).astype(jnp.bfloat16)
    return scale, tensor_scale


def quant_rows(x, peak):
    rows, cols = x.shape
    xb = x.reshape(rows // BLOCK, BLOCK, cols)
    block_max = jnp.max(jnp.abs(xb), axis=1, keepdims=True)
    scale, tensor_scale = spacing_of(block_max, peak)
    spacing = scale.astype(jnp.float32) * tensor_scale
    payload = soft_grid(xb * (1.0 / spacing)).astype(jnp.bfloat16).astype(jnp.float32)
    return (payload * spacing).reshape(rows, cols)


def quant_kernel(peak_ref, w_ref, out_ref, *, unroll):
    peak = peak_ref[0, 0]
    rows = w_ref.shape[0]

    def step(i, carry):
        sl = pl.ds(pl.multiple_of(i * BLOCK, BLOCK), BLOCK)
        out_ref[sl, :] = quant_rows(w_ref[sl, :].astype(jnp.float32), peak).astype(jnp.bfloat16)
        return carry

    lax.fori_loop(0, rows // BLOCK, step, 0, unroll=unroll)


def quant_weight(w, peak, width, first, cols):
    rows = w.shape[0]
    skip = first // width
    return pl.pallas_call(
        functools.partial(quant_kernel, unroll=4),
        grid=(cols // width,),
        in_specs=[
            pl.BlockSpec(memory_space=pltpu.SMEM),
            pl.BlockSpec((rows, width), lambda i: (0, i + skip)),
        ],
        out_specs=pl.BlockSpec((rows, width), lambda i: (0, i)),
        out_shape=jax.ShapeDtypeStruct((rows, cols), jnp.bfloat16),
        cost_estimate=pl.CostEstimate(
            flops=40 * rows * cols, bytes_accessed=4 * rows * cols, transcendentals=0
        ),
        name="quant_weight",
    )(peak, w)


def project_kernel(*refs, n_tp, n_feat, n_alias, features):
    peak_ref, act_refs = refs[0], refs[1 : 1 + n_tp]
    own_ref, peer_ref, res_ref, gain_ref, sq_in, top_in = refs[1 + n_tp : 7 + n_tp]
    refs = refs[7 + n_tp + n_alias :]
    new_ref, hid_ref, square_sum, row_top, rstd_ref, top_ref, act_q = refs
    step_id = pl.program_id(0)

    @pl.when(step_id == 0)
    def _():
        peak = peak_ref[0, 0]
        square_sum[...] = sq_in[...]
        row_top[...] = top_in[...]
        for k in range(n_tp):
            for lo in range(0, n_feat, 128):
                x = act_refs[k][lo : lo + 128, :].astype(jnp.float32)
                act_q[k, :, lo : lo + 128] = quant_rows(x, peak).T.astype(jnp.bfloat16)

    hidden = res_ref[...].astype(jnp.float32)
    for k in range(n_tp):
        w = own_ref[...] if k == 0 else peer_ref[0, k - 1]
        part = jnp.dot(act_q[k], w, preferred_element_type=jnp.float32)
        hidden = hidden + part.astype(jnp.bfloat16).astype(jnp.float32)
    new_ref[...] = hidden.astype(jnp.bfloat16)
    hid_ref[...] = hidden
    sq = square_sum[...]
    top = row_top[...]
    scaled = jnp.abs(hidden * gain_ref[...])
    for lo in range(0, hidden.shape[1], 128):
        part = hidden[:, lo : lo + 128]
        sq = sq + part * part
        top = jnp.maximum(top, scaled[:, lo : lo + 128])
    square_sum[...] = sq
    row_top[...] = top

    @pl.when(step_id == pl.num_programs(0) - 1)
    def _():
        mean_square = jnp.sum(square_sum[...], axis=1, keepdims=True) / features
        rstd = lax.rsqrt(mean_square + 1e-05)
        rstd_ref[...] = jnp.broadcast_to(rstd, rstd_ref.shape)
        top_all = jnp.max(jnp.max(row_top[...], axis=1, keepdims=True) * rstd)
        top_ref[...] = jnp.full(top_ref.shape, top_all, jnp.float32)


def project(peak, acts, w_own, w_peer, residual, gain, stats, width, skip, wide, made):
    n_tp = len(acts)
    n_feat, tokens = acts[0].shape
    d = residual.shape[1]
    steps = w_own.shape[1] // width
    column = pl.BlockSpec((tokens, width), lambda i: (0, i + skip))
    whole = pl.BlockSpec((tokens, 128), lambda i: (0, 0))
    if wide:
        peer_spec = pl.BlockSpec((1, n_tp - 1, n_feat, width), lambda i: (0, 0, 0, i))
    else:
        peer_spec = pl.BlockSpec((1, n_tp - 1, n_feat, width), lambda i: (i, 0, 0, 0))
    stat = jax.ShapeDtypeStruct((tokens, 128), jnp.float32)
    return pl.pallas_call(
        functools.partial(project_kernel, n_tp=n_tp, n_feat=n_feat, n_alias=len(made), features=d),
        grid=(steps,),
        in_specs=[pl.BlockSpec(memory_space=pltpu.SMEM)]
        + [pl.BlockSpec((n_feat, tokens), lambda i: (0, 0))] * n_tp
        + [
            pl.BlockSpec((n_feat, width), lambda i: (0, i)),
            peer_spec,
            column,
            pl.BlockSpec((1, width), lambda i: (0, i + skip)),
            whole,
            whole,
        ]
        + [pl.BlockSpec(memory_space=pl.ANY)] * len(made),
        out_specs=[column, column, whole, whole, whole, pl.BlockSpec((8, 128), lambda i: (0, 0))],
        out_shape=[
            jax.ShapeDtypeStruct((tokens, d), jnp.bfloat16),
            jax.ShapeDtypeStruct((tokens, d), jnp.float32),
            stat,
            stat,
            stat,
            jax.ShapeDtypeStruct((8, 128), jnp.float32),
        ],
        input_output_aliases={7 + n_tp + i: i for i in range(len(made))},
        scratch_shapes=[pltpu.VMEM((n_tp, tokens, n_feat), jnp.bfloat16)],
        cost_estimate=pl.CostEstimate(
            flops=2 * n_tp * n_feat * tokens * steps * width,
            bytes_accessed=2 * n_tp * n_feat * steps * width,
            transcendentals=0,
        ),
        name="project",
    )(peak, *acts, w_own, w_peer, residual, gain, *stats, *made)


def final_kernel(peak_ref, hid_ref, rstd_ref, gain_ref, out_ref, narrow, wide):
    peak = peak_ref[0, 0]
    rows, cols = hid_ref.shape
    src = lax.broadcasted_iota(jnp.int32, (128, 128), 0)
    dst = lax.broadcasted_iota(jnp.int32, (128, 128), 1)
    spread = jnp.where(src == (dst // BLOCK) * BLOCK + BLOCK - 1, 1.0, 0.0).astype(jnp.bfloat16)
    rstd = rstd_ref[...]
    tensor_scale = peak / (6.0 * 448.0)
    pieces = cols // 128
    for i in range(pieces):
        x = hid_ref[:, i * 128 : i * 128 + 128] * rstd * gain_ref[:, i * 128 : i * 128 + 128]
        m = jnp.abs(x)
        for s in (1, 2, 4, 8):
            m = jnp.maximum(m, pltpu.roll(m, s, 1))
        narrow[i * rows : (i + 1) * rows, :] = spacing_of(m, peak)[0]
    wide[...] = jnp.dot(narrow[...], spread, preferred_element_type=jnp.float32)
    for i in range(pieces):
        x = hid_ref[:, i * 128 : i * 128 + 128] * rstd * gain_ref[:, i * 128 : i * 128 + 128]
        spacing = wide[i * rows : (i + 1) * rows, :] * tensor_scale
        payload = soft_grid(x * pl.reciprocal(spacing)).astype(jnp.bfloat16).astype(jnp.float32)
        out_ref[:, i * 128 : i * 128 + 128] = (payload * spacing).astype(jnp.bfloat16)


def final_quant(peak, hidden, rstd, gain):
    tokens, d = hidden.shape
    width = 2048
    rows = min(64, tokens)
    column = pl.BlockSpec((rows, width), lambda i, j: (i, j))
    return pl.pallas_call(
        final_kernel,
        grid=(tokens // rows, d // width),
        in_specs=[
            pl.BlockSpec(memory_space=pltpu.SMEM),
            column,
            pl.BlockSpec((rows, 128), lambda i, j: (i, 0)),
            pl.BlockSpec((1, width), lambda i, j: (0, j)),
        ],
        out_specs=column,
        out_shape=jax.ShapeDtypeStruct((tokens, d), jnp.bfloat16),
        scratch_shapes=[
            pltpu.VMEM((rows * width // 128, 128), jnp.bfloat16),
            pltpu.VMEM((rows * width // 128, 128), jnp.float32),
        ],
        name="final_quant",
    )(peak, hidden, rstd, gain)


def attend(queries, keys, values, first_query):
    token_count = queries.shape[0]
    kv_heads = keys.shape[1] // HEAD_SIZE
    grouped = queries.shape[1] // HEAD_SIZE // kv_heads
    q = queries.reshape(token_count, kv_heads, grouped, HEAD_SIZE)
    k = keys.reshape(-1, kv_heads, HEAD_SIZE)
    v = values.reshape(-1, kv_heads, HEAD_SIZE)
    scores = jnp.einsum("tkgd,skd->kgts", q, k, preferred_element_type=jnp.float32)
    scores = scores * HEAD_SIZE ** (-0.5)
    query_pos = first_query + lax.broadcasted_iota(jnp.int32, (token_count, 1), 0)
    key_pos = lax.broadcasted_iota(jnp.int32, (1, k.shape[0]), 1)
    allowed = query_pos >= key_pos
    masked = jnp.where(allowed, scores, neg_large)
    top = jnp.max(masked, axis=3, keepdims=True)
    weights = jnp.where(allowed, jnp.exp(masked - top), 0.0)
    total = jnp.sum(weights, axis=3)
    summed = jnp.einsum(
        "kgts,skd->kgtd", weights.astype(jnp.bfloat16), v, preferred_element_type=jnp.float32
    )
    attended = (summed / total[..., None]).astype(jnp.bfloat16)
    return attended.transpose(0, 1, 3, 2).reshape(-1, token_count)


def peak_over(value, axes):
    return jnp.max(lax.all_gather(value.reshape(1, 1), axes)).reshape(1, 1)


def local(queries, keys, values, out_weight, residual, norm_gain):
    token_count = queries.shape[0]
    n_tp = lax.axis_size("tp")
    tp_rank = lax.axis_index("tp")
    slabs = lax.axis_size("dp") * lax.axis_size("seq")
    d = out_weight.shape[1]
    width = d // slabs
    kv = lax.all_gather(jnp.stack((keys, values)), "seq", axis=1, tiled=True)

    weight_top = jnp.max(jnp.abs(out_weight)).astype(jnp.float32)
    weight_peak = peak_over(weight_top, "tp")
    slab_id = lax.axis_index("dp") * lax.axis_size("seq") + lax.axis_index("seq")
    direct = 128
    gather_w = width - direct
    gathered = slabs * gather_w
    slab = lax.dynamic_slice_in_dim(out_weight, slab_id * gather_w, gather_w, axis=1)
    slab_q = quant_weight(slab, weight_peak, gather_w, 0, gather_w)
    shifts = [[(i, (i + k) % n_tp) for i in range(n_tp)] for k in range(1, n_tp)]
    from_peers = jnp.stack([lax.ppermute(slab_q, "tp", ring) for ring in shifts])
    w_peer = lax.all_gather(from_peers, ("dp", "seq"), axis=0)
    near_own = quant_weight(out_weight, weight_peak, 512, gathered, d - gathered)
    near_peer = jnp.stack([lax.ppermute(near_own, "tp", ring) for ring in shifts])[None]
    w_own = quant_weight(out_weight, weight_peak, gather_w, 0, gathered)

    act_t = attend(queries, kv[0], kv[1], lax.axis_index("seq") * token_count)
    act_top = jnp.max(jnp.abs(act_t)).astype(jnp.float32)
    share = token_count // n_tp
    pieces = []
    for k in range(n_tp):
        whose = lax.rem(tp_rank + k, n_tp)
        piece = lax.dynamic_slice_in_dim(act_t, whose * share, share, axis=1)
        pieces.append(piece if k == 0 else lax.ppermute(piece, "tp", shifts[k - 1]))
    act_peak = peak_over(act_top, ("seq", "tp"))

    gain = norm_gain.astype(jnp.float32).reshape(1, d)
    stats = (jnp.zeros((share, 128), jnp.float32),) * 2
    near = project(
        act_peak, pieces, near_own, near_peer, residual, gain, stats, 512, gathered // 512, True, ()
    )
    new_residual, hidden, _, _, rstd, top = project(
        act_peak, pieces, w_own, w_peer, residual, gain, near[2:4], gather_w, 0, False, near[:2]
    )
    norm_peak = peak_over(top[0, 0], ("seq", "tp"))
    next_input = final_quant(norm_peak, hidden, rstd, gain)
    return (new_residual, next_input)


def solution(mesh):
    in_specs = (
        P(("dp", "seq"), "tp"),
        P(("dp", "seq"), "tp"),
        P(("dp", "seq"), "tp"),
        P("tp", None),
        P(("dp", "seq", "tp"), None),
        P(),
    )
    out_specs = (P(("dp", "seq", "tp"), None), P(("dp", "seq", "tp"), None))
    return jax.shard_map(local, mesh=mesh, in_specs=in_specs, out_specs=out_specs, check_vma=False)
```
